32 devices in a mesh: dp: 4 (over y, z), tp: 8 (over x, core).
Axes of the slice: x: 4, y: 2, z: 2, core: 2. Of those that a mesh axis runs over, the one named last changes fastest.
The devices are a block of a 4x4x8 slice.
Arguments:
- hidden: bfloat16 [16384, 768], P(('dp', 'tp')), parts along dimension 0
- ln_gamma: float32 [768], replicated
- ln_beta: float32 [768], replicated
- out_embed: bfloat16 [51200, 768], P('tp')
- vocab_valid: int32 [51200], P('tp')
- targets: int32 [16384], P(('dp', 'tp')), parts along dimension 0
- loss_mask: int32 [16384], P(('dp', 'tp')), parts along dimension 0
Outputs:
- output 1: float32 [16384], P(('dp', 'tp')), parts along dimension 0
- output 2: float32 [4], P('dp'), parts along dimension 0
- output 3: bfloat16 [16384, 768], P(('dp', 'tp')), parts along dimension 0
- output 4: float32 [204800, 768], P(('dp', 'tp')), parts along dimension 0
- output 5: float32 [3072], P('dp'), parts along dimension 0
- output 6: float32 [3072], P('dp'), parts along dimension 0
There are 4 independent parts. The reference program is written for one: setup_inputs(seed, part) draws one part's arguments, and reference() takes and returns one part's arrays. A program takes and returns all parts, laid end to end along the dimension named above; an argument that names none is the same for every part.
All inputs are finite; a program needn't handle non-finite values.
Results may differ from the reference program's by a relative error of at most 0.001.
Values are sent between devices in bfloat16 or wider.
A program may use at most 768 MiB of HBM per device.

```python
import jax
import jax.numpy as jnp
from jax import lax

GROUP_SIZE = 8
TOKENS_DEV = 512
MODEL_DIM = 768
VOCAB_SIZE = 50257

SEQ_LEN = GROUP_SIZE * TOKENS_DEV
PAD_UNIT = 128 * GROUP_SIZE
VOCAB_PAD = (VOCAB_SIZE + PAD_UNIT - 1) // PAD_UNIT * PAD_UNIT
SHARD_VOCAB = VOCAB_PAD // GROUP_SIZE
DROP_COUNT = VOCAB_SIZE // 8
LN_EPS = 1e-5


def setup_inputs(seed: int = 0, part: int = 0) -> dict:
    base_key = jax.random.key(seed)
    k_gamma, k_beta, k_embed, k_perm = jax.random.split(base_key, 4)
    k_hidden, k_start, k_end, k_keep, k_target = jax.random.split(jax.random.fold_in(base_key, part), 5)
    hidden = jax.random.normal(k_hidden, (SEQ_LEN, MODEL_DIM), jnp.float32).astype(jnp.bfloat16)
    ln_gamma = 1.0 + 0.3 * jax.random.normal(k_gamma, (MODEL_DIM,), jnp.float32)
    ln_beta = 0.3 * jax.random.normal(k_beta, (MODEL_DIM,), jnp.float32)
    embed_scale = 2.5 * MODEL_DIM ** -0.5
    out_embed = (embed_scale * jax.random.normal(k_embed, (VOCAB_PAD, MODEL_DIM), jnp.float32)).astype(jnp.bfloat16)
    perm_ids = jax.random.permutation(k_perm, VOCAB_SIZE)
    vocab_ids = jnp.arange(VOCAB_PAD)
    vocab_valid = (vocab_ids < VOCAB_SIZE).astype(jnp.int32).at[perm_ids[:DROP_COUNT]].set(0)
    allowed_ids = perm_ids[DROP_COUNT:]
    pick_idx = jax.random.randint(k_target, (SEQ_LEN,), 0, VOCAB_SIZE - DROP_COUNT)
    targets = allowed_ids[pick_idx].astype(jnp.int32)
    positions = jnp.arange(SEQ_LEN)
    half_shard = TOKENS_DEV // 2
    start_pos = jax.random.randint(k_start, (), 0, half_shard + 1)
    end_pos = SEQ_LEN - jax.random.randint(k_end, (), 0, half_shard + 1)
    keep_tok = (jax.random.randint(k_keep, (SEQ_LEN,), 0, 4) != 0) | (positions == SEQ_LEN // 2)
    loss_mask = ((positions >= start_pos) & (positions < end_pos) & keep_tok).astype(jnp.int32)
    return {"hidden": hidden, "ln_gamma": ln_gamma, "ln_beta": ln_beta, "out_embed": out_embed, "vocab_valid": vocab_valid, "targets": targets, "loss_mask": loss_mask}


def layer_norm(hidden32, ln_gamma, ln_beta):
    row_mean = jnp.mean(hidden32, axis=-1, keepdims=True)
    centered = hidden32 - row_mean
    row_var = jnp.mean(centered * centered, axis=-1, keepdims=True)
    return centered * lax.rsqrt(row_var + LN_EPS) * ln_gamma + ln_beta


def reference(hidden, ln_gamma, ln_beta, out_embed, vocab_valid, targets, loss_mask):
    normed, ln_vjp = jax.vjp(layer_norm, hidden.astype(jnp.float32), ln_gamma, ln_beta)
    x_all = normed.astype(jnp.bfloat16)
    allowed = vocab_valid[None, :] > 0
    vocab_ids = jnp.arange(VOCAB_PAD)
    x_blocks = x_all.reshape(GROUP_SIZE, TOKENS_DEV, MODEL_DIM)
    tgt_blocks = targets.reshape(GROUP_SIZE, TOKENS_DEV)

    def token_block(block_args):
        x_blk, tgt_blk = block_args
        logits = jnp.dot(x_blk, out_embed.T, preferred_element_type=jnp.float32)
        log_norm = jax.nn.logsumexp(jnp.where(allowed, logits, -jnp.inf), axis=-1)
        picked = jnp.sum(jnp.where(vocab_ids[None, :] == tgt_blk[:, None], logits, 0.0), axis=-1)
        return log_norm, picked

    log_norm, picked = lax.map(token_block, (x_blocks, tgt_blocks))
    log_norm = log_norm.reshape(SEQ_LEN)
    picked = picked.reshape(SEQ_LEN)
    weight = loss_mask.astype(jnp.float32)
    tok_count = jnp.sum(weight)
    tok_loss = (log_norm - picked) * weight
    mean_loss = jnp.sum(tok_loss) / tok_count
    tok_scale = weight / tok_count

    embed_shards = out_embed.reshape(GROUP_SIZE, SHARD_VOCAB, MODEL_DIM)
    valid_shards = vocab_valid.reshape(GROUP_SIZE, SHARD_VOCAB)
    shard_start = jnp.arange(GROUP_SIZE) * SHARD_VOCAB

    def vocab_block(dx_acc, block_args):
        emb_blk, valid_blk, offset = block_args
        logits = jnp.dot(x_all, emb_blk.T, preferred_element_type=jnp.float32)
        soft_probs = jnp.where(valid_blk[None, :] > 0, jnp.exp(logits - log_norm[:, None]), 0.0)
        target_hit = (offset + jnp.arange(SHARD_VOCAB))[None, :] == targets[:, None]
        d_logits = ((soft_probs - target_hit.astype(jnp.float32)) * tok_scale[:, None]).astype(jnp.bfloat16)
        d_emb = jnp.dot(d_logits.T, x_all, preferred_element_type=jnp.float32)
        dx_acc = dx_acc + jnp.dot(d_logits, emb_blk, preferred_element_type=jnp.float32)
        return dx_acc, d_emb

    dx_all, d_embed = lax.scan(vocab_block, jnp.zeros((SEQ_LEN, MODEL_DIM), jnp.float32), (embed_shards, valid_shards, shard_start))
    d_embed = d_embed.reshape(VOCAB_PAD, MODEL_DIM)
    d_hidden, d_gamma, d_beta = ln_vjp(dx_all)
    return tok_loss, mean_loss.reshape(1), d_hidden.astype(jnp.bfloat16), d_embed, d_gamma, d_beta
```

```python
import functools

import jax
import jax.numpy as jnp
from jax import lax
from jax.experimental import pallas as pl
from jax.experimental.pallas import tpu as pltpu
from jax.sharding import PartitionSpec as P

LN_EPS = 1e-5
LOG2E = 1.4426950408889634
LN2 = 0.6931471805599453
LOW = -3.0e38
TV = 1280
TT = 512
ANY = pl.BlockSpec(memory_space=pl.ANY)
VM = pl.BlockSpec(memory_space=pltpu.VMEM)
VMEM_LIMIT = 64000 * 1024


def layer_norm(hidden32, ln_gamma, ln_beta):
    row_mean = jnp.mean(hidden32, axis=-1, keepdims=True)
    centered = hidden32 - row_mean
    row_var = jnp.mean(centered * centered, axis=-1, keepdims=True)
    return centered * lax.rsqrt(row_var + LN_EPS) * ln_gamma + ln_beta


def cols(start, size=TT):
    return pl.ds(pl.multiple_of(start, 128), size)


def tile_stats(z_ref, base, col, tgt_ref, m_ref, s_ref, p_ref):
    rows, tokens = z_ref.shape
    at = cols(col, tokens)
    rel = jnp.broadcast_to(tgt_ref[:, at], (8, tokens)) - lax.broadcasted_iota(jnp.int32, (8, tokens), 0) - base
    m_old = m_ref[:, at]
    m_new = m_old
    for r in range(0, rows, 8):
        m_new = jnp.maximum(m_new, z_ref[r:r + 8])
    s = s_ref[:, at] * jnp.exp2(m_old - m_new)
    picked = p_ref[:, at]
    for r in range(0, rows, 8):
        z = z_ref[r:r + 8]
        s = s + jnp.exp2(z - m_new)
        picked = picked + jnp.where(rel == r, z, 0.0)
    m_ref[:, at] = m_new
    s_ref[:, at] = s
    p_ref[:, at] = picked


def forward_kernel(e_ref, bias_ref, x_ref, tgt_ref, z_hbm, m_ref, s_ref, p_ref, *rest):
    nv, nt = e_ref.shape[0] // TV, x_ref.shape[0] // TT
    zb, out_sem = rest[:nv], rest[nv]
    m_ref[...] = jnp.full(m_ref.shape, LOW, jnp.float32)
    s_ref[...] = jnp.zeros(s_ref.shape, jnp.float32)
    p_ref[...] = jnp.zeros(p_ref.shape, jnp.float32)
    zb[-1][...] = jnp.full(zb[-1].shape, -jnp.inf, jnp.float32)

    def out(k, t):
        return pltpu.make_async_copy(zb[k], z_hbm.at[t * nv + k], out_sem.at[k])

    for k in range(nv):
        out(k, 0).start()

    def body(t, carry):
        x_blk = x_ref[pl.ds(pl.multiple_of(t * TT, TT), TT), :]
        for v in range(nv):
            out(v, 0).wait()
            at = slice(v * TV, (v + 1) * TV)
            z = lax.dot_general(e_ref[at, :], x_blk, (((1,), (1,)), ((), ())), preferred_element_type=jnp.float32)
            zb[v][...] = z * LOG2E + jnp.concatenate([bias_ref[at, :]] * (TT // 128), axis=1)
            prev = (v - 1) % nv
            t_prev = t if v else jnp.maximum(t - 1, 0)
            base = prev * TV if v else jnp.where(t > 0, prev * TV, -(1 << 30))
            tile_stats(zb[prev], base, t_prev * TT, tgt_ref, m_ref, s_ref, p_ref)
            out(v, t).start()
        return carry

    lax.fori_loop(0, nt, body, 0)
    tile_stats(zb[-1], (nv - 1) * TV, (nt - 1) * TT, tgt_ref, m_ref, s_ref, p_ref)
    for k in range(nv):
        out(k, 0).wait()


def forward(embed, bias, x_all, tgt):
    v, t, d = embed.shape[0], x_all.shape[0], x_all.shape[1]
    nv = v // TV
    stat = jax.ShapeDtypeStruct((8, t), jnp.float32)
    return pl.pallas_call(
        forward_kernel,
        out_shape=(jax.ShapeDtypeStruct((nv * (t // TT), TV, TT), jnp.float32), stat, stat, stat),
        in_specs=[VM] * 4,
        out_specs=(ANY, VM, VM, VM),
        scratch_shapes=[pltpu.VMEM((TV, TT), jnp.float32)] * nv + [pltpu.SemaphoreType.DMA((nv,))],
        compiler_params=pltpu.CompilerParams(vmem_limit_bytes=VMEM_LIMIT),
        cost_estimate=pl.CostEstimate(flops=2 * v * t * d, bytes_accessed=4 * v * t, transcendentals=v * t),
        name="logits",
    )(embed, bias, x_all, tgt)


def tile_grad(z_ref, dz_ref, base, col, lse_ref, w_ref, tgt_ref):
    rows, tokens = z_ref.shape
    for c in range(0, tokens, 128):
        at = cols(col + c, 128)
        lse = jnp.broadcast_to(lse_ref[:, at], (8, 128))
        w = jnp.broadcast_to(w_ref[:, at], (8, 128))
        rel = jnp.broadcast_to(tgt_ref[:, at], (8, 128)) - lax.broadcasted_iota(jnp.int32, (8, 128), 0) - base
        for r in range(0, rows, 16):
            pair = []
            for q in (r, r + 8):
                p = jnp.exp2(z_ref[q:q + 8, c:c + 128] - lse)
                pair.append(p - jnp.where(rel == q, w, 0.0))
            dz_ref[r:r + 16, c:c + 128] = jnp.concatenate(pair, axis=0).astype(jnp.bfloat16)


def dx_kernel(et_ref, lse_ref, w_ref, tgt_ref, z_hbm, dx_hbm, *rest):
    nv, nt = et_ref.shape[1] // TV, lse_ref.shape[1] // TT
    n = nv * nt
    zb, db = rest[:nv], rest[nv:nv + 2]
    acc, z_sem, x_sem = rest[nv + 2:]

    def z_in(k, g):
        return pltpu.make_async_copy(z_hbm.at[g], zb[k], z_sem.at[k])

    def x_out(par, t):
        return pltpu.make_async_copy(acc.at[par], dx_hbm.at[t], x_sem.at[par])

    def grad(v, t, d_ref):
        tile_grad(zb[v], d_ref, v * TV, t * TT, lse_ref, w_ref, tgt_ref)

    for k in range(nv):
        z_in(k, k).start()
    for k in range(2):
        x_out(k, k).start()
    z_in(0, 0).wait()
    grad(0, 0, db[0])
    z_in(0, nv).start()

    def block(t, par):
        x_out(par, 0).wait()
        for v in range(nv):
            cur, nxt = db[(par * nv + v) % 2], db[(par * nv + v + 1) % 2]
            vn = (v + 1) % nv
            tn = t if v + 1 < nv else jnp.minimum(t + 1, nt - 1)
            z_in(vn, 0).wait()
            d = jnp.dot(et_ref[:, v * TV:(v + 1) * TV], cur[...], preferred_element_type=jnp.float32)
            acc[par] = d if v == 0 else acc[par] + d
            grad(vn, tn, nxt)
            z_in(vn, jnp.minimum((tn + 1) * nv + vn, n - nv + vn)).start()
        x_out(par, t).start()

    def body(i, carry):
        block(2 * i, 0)
        block(2 * i + 1, 1)
        return carry

    lax.fori_loop(0, nt // 2, body, 0)
    for k in range(nv):
        z_in(k, 0).wait()
    for k in range(2):
        x_out(k, 0).wait()


def token_grad(embed_t, lse, w, tgt, z):
    (d, v), t = embed_t.shape, lse.shape[1]
    nv = v // TV
    return pl.pallas_call(
        dx_kernel,
        out_shape=jax.ShapeDtypeStruct((t // TT, d, TT), jnp.float32),
        in_specs=[VM] * 4 + [ANY],
        out_specs=ANY,
        scratch_shapes=[pltpu.VMEM((TV, TT), jnp.float32)] * nv
        + [pltpu.VMEM((TV, TT), jnp.bfloat16)] * 2
        + [pltpu.VMEM((2, d, TT), jnp.float32), pltpu.SemaphoreType.DMA((nv,)), pltpu.SemaphoreType.DMA((2,))],
        compiler_params=pltpu.CompilerParams(vmem_limit_bytes=VMEM_LIMIT),
        cost_estimate=pl.CostEstimate(flops=2 * v * t * d, bytes_accessed=4 * v * t, transcendentals=v * t),
        name="token_grad",
    )(embed_t, lse, w, tgt, z)


def de_kernel(z_ref, x_ref, lse_ref, w_ref, tgt_ref, o_ref):
    v, t = pl.program_id(0), pl.program_id(1)
    at = cols(t * TT)
    lse = lse_ref[:, at]
    w = jnp.broadcast_to(w_ref[:, at], (8, TT))
    rel = jnp.broadcast_to(tgt_ref[:, at], (8, TT)) - lax.broadcasted_iota(jnp.int32, (8, TT), 0) - v * TV
    x_blk = x_ref[pl.ds(pl.multiple_of(t * TT, TT), TT), :]

    @pl.when(t == 0)
    def _():
        o_ref[...] = jnp.zeros_like(o_ref)

    for k in range(0, TV, 256):
        p = jnp.exp2(z_ref[0, k:k + 256] - lse)
        dz = jnp.concatenate([p[r:r + 8] - jnp.where(rel == k + r, w, 0.0) for r in range(0, 256, 8)], axis=0)
        o_ref[k:k + 256] += jnp.dot(dz.astype(jnp.bfloat16), x_blk, preferred_element_type=jnp.float32)


def embed_grad(z, x_all, lse, w, tgt, v):
    t, d = x_all.shape
    nv = v // TV
    return pl.pallas_call(
        de_kernel,
        grid=(nv, t // TT),
        out_shape=jax.ShapeDtypeStruct((v, d), jnp.float32),
        in_specs=[pl.BlockSpec((1, TV, TT), lambda i, j: (j * nv + i, 0, 0))] + [VM] * 4,
        out_specs=pl.BlockSpec((TV, d), lambda i, j: (i, 0)),
        compiler_params=pltpu.CompilerParams(vmem_limit_bytes=VMEM_LIMIT),
        cost_estimate=pl.CostEstimate(flops=2 * v * t * d, bytes_accessed=4 * v * t + 4 * v * d, transcendentals=v * t),
        name="embed_grad",
    )(z, x_all, lse, w, tgt)


def norm_grad_kernel(h_ref, gamma_ref, dxt_ref, dh_ref, g_ref):
    h = h_ref[...].astype(jnp.float32)
    mean = jnp.mean(h, axis=1, keepdims=True)
    cen = h - mean
    rstd = lax.rsqrt(jnp.mean(cen * cen, axis=1, keepdims=True) + LN_EPS)
    xhat = cen * rstd
    dy = dxt_ref[...].T
    g_ref[0:1, :] = jnp.sum(dy * xhat, axis=0, keepdims=True)
    g_ref[1:2, :] = jnp.sum(dy, axis=0, keepdims=True)
    dn = dy * gamma_ref[...]
    dh = rstd * (dn - jnp.mean(dn, axis=1, keepdims=True) - xhat * jnp.mean(dn * xhat, axis=1, keepdims=True))
    dh_ref[...] = dh.astype(jnp.bfloat16)


def norm_grad(hidden, gamma, dx_t):
    t, d = hidden.shape
    return pl.pallas_call(
        norm_grad_kernel,
        out_shape=(jax.ShapeDtypeStruct((t, d), jnp.bfloat16), jax.ShapeDtypeStruct((2, d), jnp.float32)),
        in_specs=[VM] * 3,
        out_specs=(VM, VM),
        compiler_params=pltpu.CompilerParams(vmem_limit_bytes=VMEM_LIMIT),
        name="norm_grad",
    )(hidden, gamma[None, :], dx_t)


def solution(mesh):
    tok_spec = P(("dp", "tp"))
    row_spec = P(("dp", "tp"), None)

    def local_step(hidden_blk, ln_gamma, ln_beta, embed_blk, valid_blk, tgt_blk, mask_blk):
        tok_local = hidden_blk.shape[0]
        shard_vocab = embed_blk.shape[0]
        shard_idx = lax.axis_index("tp")
        normed = layer_norm(hidden_blk.astype(jnp.float32), ln_gamma, ln_beta)
        x_all = lax.all_gather(normed.astype(jnp.bfloat16), "tp", axis=0, tiled=True)
        labels = lax.all_gather(jnp.stack([tgt_blk, mask_blk]), "tp", axis=1, tiled=True)
        weight = labels[1].astype(jnp.float32)
        tok_count = jnp.sum(weight)
        tgt = (labels[0] - shard_idx * shard_vocab)[None, :]
        bias = jnp.broadcast_to(jnp.where(valid_blk > 0, 0.0, -jnp.inf)[:, None], (shard_vocab, 128))
        z, m8, s8, p8 = forward(embed_blk, bias, x_all, tgt)
        m1 = jnp.max(m8, axis=0)
        part = jnp.stack([m1, jnp.sum(s8 * jnp.exp2(m8 - m1), axis=0), jnp.sum(p8, axis=0)])
        parts = lax.all_gather(part, "tp", axis=0)
        row_max = jnp.max(parts[:, 0], axis=0)
        lse2 = row_max + jnp.log2(jnp.sum(parts[:, 1] * jnp.exp2(parts[:, 0] - row_max), axis=0))
        tok_loss = (lse2 - jnp.sum(parts[:, 2], axis=0)) * LN2 * weight
        mean_loss = (jnp.sum(tok_loss) / tok_count).reshape(1)
        shift = jnp.where(weight > 0, lse2 + jnp.log2(tok_count), jnp.inf)[None, :]
        scale = (weight / tok_count)[None, :]
        dx_part = token_grad(embed_blk.T, shift, scale, tgt, z)
        dx_local = lax.psum_scatter(dx_part, "tp", scatter_dimension=0, tiled=False)
        d_embed = embed_grad(z, x_all, shift, scale, tgt, shard_vocab)
        d_hidden, ln_part = norm_grad(hidden_blk, ln_gamma, dx_local)
        ln_grads = lax.psum(ln_part, "tp")
        loss_local = lax.dynamic_slice_in_dim(tok_loss, shard_idx * tok_local, tok_local)
        return loss_local, mean_loss, d_hidden, d_embed, ln_grads[0], ln_grads[1]

    return jax.shard_map(local_step, mesh=mesh, in_specs=(row_spec, P(), P(), P("tp", None), P("tp"), tok_spec, tok_spec), out_specs=(tok_spec, P("dp"), row_spec, row_spec, P("dp"), P("dp")), check_vma=False)
```

```python
import functools

import jax
import jax.numpy as jnp
from jax import lax
from jax.experimental import pallas as pl
from jax.experimental.pallas import tpu as pltpu
from jax.sharding import PartitionSpec as P

LN_EPS = 1e-5
LOG2E = 1.4426950408889634
LN2 = 0.6931471805599453
LOW = -3.0e38
TV = 1280
TT = 512
ANY = pl.BlockSpec(memory_space=pl.ANY)
VM = pl.BlockSpec(memory_space=pltpu.VMEM)
VMEM_LIMIT = 64000 * 1024


def layer_norm(hidden32, ln_gamma, ln_beta):
    row_mean = jnp.mean(hidden32, axis=-1, keepdims=True)
    centered = hidden32 - row_mean
    row_var = jnp.mean(centered * centered, axis=-1, keepdims=True)
    return centered * lax.rsqrt(row_var + LN_EPS) * ln_gamma + ln_beta


def cols(start, size=TT):
    return pl.ds(pl.multiple_of(start, 128), size)


def tile_stats(z_ref, base, col, tgt_ref, m_ref, s_ref, p_ref):
    rows, tokens = z_ref.shape
    at = cols(col, tokens)
    rel = jnp.broadcast_to(tgt_ref[:, at], (8, tokens)) - lax.broadcasted_iota(jnp.int32, (8, tokens), 0) - base
    m_old = m_ref[:, at]
    m_new = m_old
    for r in range(0, rows, 8):
        m_new = jnp.maximum(m_new, z_ref[r:r + 8])
    s = s_ref[:, at] * jnp.exp2(m_old - m_new)
    picked = p_ref[:, at]
    for r in range(0, rows, 8):
        z = z_ref[r:r + 8]
        s = s + jnp.exp2(z - m_new)
        picked = picked + jnp.where(rel == r, z, 0.0)
    m_ref[:, at] = m_new
    s_ref[:, at] = s
    p_ref[:, at] = picked


def forward_kernel(e_hbm, keep_ref, x_hbm, tgt_ref, z_hbm, m_ref, s_ref, p_ref, e_ref, x_ref, bias_ref, *rest):
    nv, nt = e_ref.shape[0] // TV, x_ref.shape[0]
    zb, (out_sem, e_sem, x_sem) = rest[:nv], rest[nv:]

    def load_e(v):
        at = pl.ds(v * TV, TV)
        return pltpu.make_async_copy(e_hbm.at[at], e_ref.at[at], e_sem.at[v])

    def load_x(t):
        return pltpu.make_async_copy(x_hbm.at[t, pl.ds(0, TT)], x_ref.at[t], x_sem.at[t])

    load_x(0).start()
    for v in range(nv):
        load_e(v).start()
    for t in range(1, nt):
        load_x(t).start()
    m_ref[...] = jnp.full(m_ref.shape, LOW, jnp.float32)
    s_ref[...] = jnp.zeros(s_ref.shape, jnp.float32)
    p_ref[...] = jnp.zeros(p_ref.shape, jnp.float32)
    zb[-1][...] = jnp.full(zb[-1].shape, -jnp.inf, jnp.float32)
    for j in range(keep_ref.shape[0]):
        bias_ref[j * 128:(j + 1) * 128, :] = jnp.broadcast_to(keep_ref[j:j + 1, :], (128, 128)).T

    def out(k, t):
        return pltpu.make_async_copy(zb[k], z_hbm.at[t * nv + k], out_sem.at[k])

    def body(t, carry):
        load_x(t).wait()
        x_blk = x_ref[t]
        for v in range(nv):
            @pl.when(t == 0)
            def _():
                load_e(v).wait()

            @pl.when(t > 0)
            def _():
                out(v, 0).wait()

            at = slice(v * TV, (v + 1) * TV)
            z = lax.dot_general(e_ref[at, :], x_blk, (((1,), (1,)), ((), ())), preferred_element_type=jnp.float32)
            zb[v][...] = z * LOG2E + jnp.concatenate([bias_ref[at, :]] * (TT // 128), axis=1)
            prev = (v - 1) % nv
            t_prev = t if v else jnp.maximum(t - 1, 0)
            base = prev * TV if v else jnp.where(t > 0, prev * TV, -(1 << 30))
            tile_stats(zb[prev], base, t_prev * TT, tgt_ref, m_ref, s_ref, p_ref)
            out(v, t).start()
        return carry

    lax.fori_loop(0, nt, body, 0)
    tile_stats(zb[-1], (nv - 1) * TV, (nt - 1) * TT, tgt_ref, m_ref, s_ref, p_ref)
    for k in range(nv):
        out(k, 0).wait()


def forward(embed, keep, x_all, tgt):
    (v, d), nt = embed.shape, x_all.shape[0]
    t, nv = nt * TT, v // TV
    stat = jax.ShapeDtypeStruct((8, t), jnp.float32)
    return pl.pallas_call(
        forward_kernel,
        out_shape=(jax.ShapeDtypeStruct((nv * nt, TV, TT), jnp.float32), stat, stat, stat),
        in_specs=[ANY, VM, ANY, VM],
        out_specs=(ANY, VM, VM, VM),
        scratch_shapes=[
            pltpu.VMEM((v, d), jnp.bfloat16),
            pltpu.VMEM((nt, TT, d), jnp.bfloat16),
            pltpu.VMEM((v, 128), jnp.float32),
        ]
        + [pltpu.VMEM((TV, TT), jnp.float32)] * nv
        + [pltpu.SemaphoreType.DMA((nv,)), pltpu.SemaphoreType.DMA((nv,)), pltpu.SemaphoreType.DMA((nt,))],
        compiler_params=pltpu.CompilerParams(vmem_limit_bytes=VMEM_LIMIT),
        cost_estimate=pl.CostEstimate(flops=2 * v * t * d, bytes_accessed=4 * v * t, transcendentals=v * t),
        name="logits",
    )(embed, keep, x_all, tgt)


def tile_grad(z_ref, dz_ref, base, col, lse_ref, w_ref, tgt_ref):
    rows, tokens = z_ref.shape
    for c in range(0, tokens, 128):
        at = cols(col + c, 128)
        lse = jnp.broadcast_to(lse_ref[:, at], (8, 128))
        w = jnp.broadcast_to(w_ref[:, at], (8, 128))
        rel = jnp.broadcast_to(tgt_ref[:, at], (8, 128)) - lax.broadcasted_iota(jnp.int32, (8, 128), 0) - base
        for r in range(0, rows, 16):
            pair = []
            for q in (r, r + 8):
                p = jnp.exp2(z_ref[q:q + 8, c:c + 128] - lse)
                pair.append(p - jnp.where(rel == q, w, 0.0))
            dz_ref[r:r + 16, c:c + 128] = jnp.concatenate(pair, axis=0).astype(jnp.bfloat16)


def dx_kernel(et_ref, lse_ref, w_ref, tgt_ref, z_hbm, dx_hbm, *rest):
    nv, nt = et_ref.shape[1] // TV, lse_ref.shape[1] // TT
    n = nv * nt
    zb, db = rest[:nv], rest[nv:nv + 2]
    acc, z_sem, x_sem = rest[nv + 2:]

    def z_in(k, g):
        return pltpu.make_async_copy(z_hbm.at[g], zb[k], z_sem.at[k])

    def x_out(par, t):
        return pltpu.make_async_copy(acc.at[par], dx_hbm.at[t], x_sem.at[par])

    def grad(v, t, d_ref):
        tile_grad(zb[v], d_ref, v * TV, t * TT, lse_ref, w_ref, tgt_ref)

    for k in range(nv):
        z_in(k, k).start()
    for k in range(2):
        x_out(k, k).start()
    z_in(0, 0).wait()
    grad(0, 0, db[0])
    z_in(0, nv).start()

    def block(t, par):
        x_out(par, 0).wait()
        for v in range(nv):
            cur, nxt = db[(par * nv + v) % 2], db[(par * nv + v + 1) % 2]
            vn = (v + 1) % nv
            tn = t if v + 1 < nv else jnp.minimum(t + 1, nt - 1)
            z_in(vn, 0).wait()
            d = jnp.dot(et_ref[:, v * TV:(v + 1) * TV], cur[...], preferred_element_type=jnp.float32)
            acc[par] = d if v == 0 else acc[par] + d
            grad(vn, tn, nxt)
            z_in(vn, jnp.minimum((tn + 1) * nv + vn, n - nv + vn)).start()
        x_out(par, t).start()

    def body(i, carry):
        block(2 * i, 0)
        block(2 * i + 1, 1)
        return carry

    lax.fori_loop(0, nt // 2, body, 0)
    for k in range(nv):
        z_in(k, 0).wait()
    for k in range(2):
        x_out(k, 0).wait()


def token_grad(embed_t, lse, w, tgt, z):
    (d, v), t = embed_t.shape, lse.shape[1]
    nv = v // TV
    return pl.pallas_call(
        dx_kernel,
        out_shape=jax.ShapeDtypeStruct((t // TT, d, TT), jnp.float32),
        in_specs=[VM] * 4 + [ANY],
        out_specs=ANY,
        scratch_shapes=[pltpu.VMEM((TV, TT), jnp.float32)] * nv
        + [pltpu.VMEM((TV, TT), jnp.bfloat16)] * 2
        + [pltpu.VMEM((2, d, TT), jnp.float32), pltpu.SemaphoreType.DMA((nv,)), pltpu.SemaphoreType.DMA((2,))],
        compiler_params=pltpu.CompilerParams(vmem_limit_bytes=VMEM_LIMIT),
        cost_estimate=pl.CostEstimate(flops=2 * v * t * d, bytes_accessed=4 * v * t, transcendentals=v * t),
        name="token_grad",
    )(embed_t, lse, w, tgt, z)


def de_kernel(z_hbm, x_ref, lse_ref, w_ref, tgt_ref, o_hbm, acc, *rest):
    nt = x_ref.shape[0]
    nv = z_hbm.shape[0] // nt
    zb, (z_sem, o_sem) = rest[:4], rest[4:]

    def z_in(k, g):
        v, t = lax.div(g, nt // 4), lax.rem(g, nt // 4) * 4 + k
        return pltpu.make_async_copy(z_hbm.at[t * nv + v], zb[k], z_sem.at[k])

    def o_out(v):
        return pltpu.make_async_copy(acc.at[lax.rem(v, 2)], o_hbm.at[pl.ds(pl.multiple_of(v * TV, TV), TV)], o_sem.at[lax.rem(v, 2)])

    for k in range(4):
        z_in(k, 0).start()
    last = nv * (nt // 4) - 1

    def body(g, carry):
        v, q = lax.div(g, nt // 4), lax.rem(g, nt // 4)
        slot = lax.rem(v, 2)

        @pl.when((q == 0) & (v >= 2))
        def _():
            o_out(v).wait()

        for k in range(4):
            z_in(k, 0).wait()
            t = q * 4 + k
            at = cols(t * TT)
            lse = lse_ref[:, at]
            w = jnp.broadcast_to(w_ref[:, at], (8, TT))
            rel = jnp.broadcast_to(tgt_ref[:, at], (8, TT)) - lax.broadcasted_iota(jnp.int32, (8, TT), 0) - v * TV
            x_blk = x_ref[t, :TT]
            for c in range(0, TV, 256):
                p = jnp.exp2(zb[k][c:c + 256] - lse)
                dz = jnp.concatenate([p[r:r + 8] - jnp.where(rel == c + r, w, 0.0) for r in range(0, 256, 8)], axis=0)
                d = jnp.dot(dz.astype(jnp.bfloat16), x_blk, preferred_element_type=jnp.float32)
                old = acc[slot, c:c + 256]
                acc[slot, c:c + 256] = d + (jnp.where(q == 0, 0.0, old) if k == 0 else old)
            z_in(k, jnp.minimum(g + 1, last)).start()

        @pl.when(q == nt // 4 - 1)
        def _():
            o_out(v).start()

        return carry

    lax.fori_loop(0, last + 1, body, 0)
    for k in range(4):
        z_in(k, 0).wait()
    for v in range(max(nv - 2, 0), nv):
        o_out(v).wait()


def embed_grad(z, x_all, lse, w, tgt, v):
    nt, _, d = x_all.shape
    t = nt * TT
    return pl.pallas_call(
        de_kernel,
        out_shape=jax.ShapeDtypeStruct((v, d), jnp.float32),
        in_specs=[ANY] + [VM] * 4,
        out_specs=ANY,
        scratch_shapes=[pltpu.VMEM((2, TV, d), jnp.float32)]
        + [pltpu.VMEM((TV, TT), jnp.float32)] * 4
        + [pltpu.SemaphoreType.DMA((4,)), pltpu.SemaphoreType.DMA((2,))],
        compiler_params=pltpu.CompilerParams(vmem_limit_bytes=VMEM_LIMIT),
        cost_estimate=pl.CostEstimate(flops=2 * v * t * d, bytes_accessed=4 * v * t + 4 * v * d, transcendentals=v * t),
        name="embed_grad",
    )(z, x_all, lse, w, tgt)


def norm_grad_kernel(h_ref, gamma_ref, dxt_ref, dh_ref, g_ref):
    h = h_ref[...].astype(jnp.float32)
    mean = jnp.mean(h, axis=1, keepdims=True)
    cen = h - mean
    rstd = lax.rsqrt(jnp.mean(cen * cen, axis=1, keepdims=True) + LN_EPS)
    xhat = cen * rstd
    dy = dxt_ref[...].T
    g_ref[0:1, :] = jnp.sum(dy * xhat, axis=0, keepdims=True)
    g_ref[1:2, :] = jnp.sum(dy, axis=0, keepdims=True)
    dn = dy * gamma_ref[...]
    dh = rstd * (dn - jnp.mean(dn, axis=1, keepdims=True) - xhat * jnp.mean(dn * xhat, axis=1, keepdims=True))
    dh_ref[...] = dh.astype(jnp.bfloat16)


def norm_grad(hidden, gamma, dx_t):
    t, d = hidden.shape
    return pl.pallas_call(
        norm_grad_kernel,
        out_shape=(jax.ShapeDtypeStruct((t, d), jnp.bfloat16), jax.ShapeDtypeStruct((2, d), jnp.float32)),
        in_specs=[VM] * 3,
        out_specs=(VM, VM),
        compiler_params=pltpu.CompilerParams(vmem_limit_bytes=VMEM_LIMIT),
        name="norm_grad",
    )(hidden, gamma[None, :], dx_t)


def solution(mesh):
    tok_spec = P(("dp", "tp"))
    row_spec = P(("dp", "tp"), None)

    def local_step(hidden_blk, ln_gamma, ln_beta, embed_blk, valid_blk, tgt_blk, mask_blk):
        tok_local = hidden_blk.shape[0]
        shard_vocab = embed_blk.shape[0]
        shard_idx = lax.axis_index("tp")
        normed = layer_norm(hidden_blk.astype(jnp.float32), ln_gamma, ln_beta)
        label_rows = jnp.stack([tgt_blk // 256, tgt_blk % 256, mask_blk]).astype(jnp.bfloat16)
        label_rows = jnp.pad(label_rows, ((0, 16 - label_rows.shape[0]), (0, hidden_blk.shape[1] - tok_local)))
        packed = jnp.concatenate([normed.astype(jnp.bfloat16), label_rows], axis=0)
        x_all = lax.all_gather(packed, "tp", axis=0)
        labels = x_all[:, tok_local:tok_local + 3, :tok_local].astype(jnp.float32)
        weight = labels[:, 2].reshape(-1)
        tok_count = jnp.sum(weight)
        target_ids = (labels[:, 0] * 256.0 + labels[:, 1]).astype(jnp.int32).reshape(-1)
        tgt = (target_ids - shard_idx * shard_vocab)[None, :]
        keep = jnp.where(valid_blk > 0, 0.0, -jnp.inf).reshape(-1, 128)
        z, m8, s8, p8 = forward(embed_blk, keep, x_all, tgt)
        m1 = jnp.max(m8, axis=0)
        part = jnp.stack([m1, jnp.sum(s8 * jnp.exp2(m8 - m1), axis=0), jnp.sum(p8, axis=0)])
        parts = lax.all_gather(part, "tp", axis=0)
        row_max = jnp.max(parts[:, 0], axis=0)
        lse2 = row_max + jnp.log2(jnp.sum(parts[:, 1] * jnp.exp2(parts[:, 0] - row_max), axis=0))
        tok_loss = (lse2 - jnp.sum(parts[:, 2], axis=0)) * LN2 * weight
        mean_loss = (jnp.sum(tok_loss) / tok_count).reshape(1)
        shift = jnp.where(weight > 0, lse2 + jnp.log2(tok_count), jnp.inf)[None, :]
        scale = (weight / tok_count)[None, :]
        dx_part = token_grad(embed_blk.T, shift, scale, tgt, z)
        dx_local = lax.psum_scatter(dx_part, "tp", scatter_dimension=0, tiled=False)
        d_embed = embed_grad(z, x_all, shift, scale, tgt, shard_vocab)
        d_hidden, ln_part = norm_grad(hidden_blk, ln_gamma, dx_local)
        ln_grads = lax.psum(ln_part, "tp")
        loss_local = lax.dynamic_slice_in_dim(tok_loss, shard_idx * tok_local, tok_local)
        return loss_local, mean_loss, d_hidden, d_embed, ln_grads[0], ln_grads[1]

    return jax.shard_map(local_step, mesh=mesh, in_specs=(row_spec, P(), P(), P("tp", None), P("tp"), tok_spec, tok_spec), out_specs=(tok_spec, P("dp"), row_spec, row_spec, P("dp"), P("dp")), check_vma=False)
```

```python
import functools

import jax
import jax.numpy as jnp
from jax import lax
from jax.experimental import pallas as pl
from jax.experimental.pallas import tpu as pltpu
from jax.sharding import PartitionSpec as P

LN_EPS = 1e-5
LOG2E = 1.4426950408889634
LN2 = 0.6931471805599453
LOW = -3.0e38
TV = 1280
TT = 512
ANY = pl.BlockSpec(memory_space=pl.ANY)
VM = pl.BlockSpec(memory_space=pltpu.VMEM)
VMEM_LIMIT = 64000 * 1024


def layer_norm(hidden32, ln_gamma, ln_beta):
    row_mean = jnp.mean(hidden32, axis=-1, keepdims=True)
    centered = hidden32 - row_mean
    row_var = jnp.mean(centered * centered, axis=-1, keepdims=True)
    return centered * lax.rsqrt(row_var + LN_EPS) * ln_gamma + ln_beta


def cols(start, size=TT):
    return pl.ds(pl.multiple_of(start, 128), size)


def tile_stats(z_ref, base, col, tgt_ref, m_ref, s_ref, p_ref):
    rows, tokens = z_ref.shape
    at = cols(col, tokens)
    rel = jnp.broadcast_to(tgt_ref[:, at], (8, tokens)) - lax.broadcasted_iota(jnp.int32, (8, tokens), 0) - base
    m_old = m_ref[:, at]
    m_new = m_old
    for r in range(0, rows, 8):
        m_new = jnp.maximum(m_new, z_ref[r:r + 8])
    s = s_ref[:, at] * jnp.exp2(m_old - m_new)
    picked = p_ref[:, at]
    for r in range(0, rows, 8):
        z = z_ref[r:r + 8]
        s = s + jnp.exp2(z - m_new)
        picked = picked + jnp.where(rel == r, z, 0.0)
    m_ref[:, at] = m_new
    s_ref[:, at] = s
    p_ref[:, at] = picked


def forward_kernel(e_hbm, keep_ref, x_hbm, tgt_ref, z_hbm, m_ref, s_ref, p_ref, e_ref, x_ref, bias_ref, *rest):
    nv, nt = e_ref.shape[0] // TV, x_ref.shape[0]
    zb, (out_sem, e_sem, x_sem) = rest[:nv], rest[nv:]

    def load_e(v):
        at = pl.ds(v * TV, TV)
        return pltpu.make_async_copy(e_hbm.at[at], e_ref.at[at], e_sem.at[v])

    def load_x(t):
        return pltpu.make_async_copy(x_hbm.at[t, pl.ds(0, TT)], x_ref.at[t], x_sem.at[t])

    load_x(0).start()
    for v in range(nv):
        load_e(v).start()
    for t in range(1, nt):
        load_x(t).start()
    m_ref[...] = jnp.full(m_ref.shape, LOW, jnp.float32)
    s_ref[...] = jnp.zeros(s_ref.shape, jnp.float32)
    p_ref[...] = jnp.zeros(p_ref.shape, jnp.float32)
    zb[-1][...] = jnp.full(zb[-1].shape, -jnp.inf, jnp.float32)
    for j in range(keep_ref.shape[0]):
        bias_ref[j * 128:(j + 1) * 128, :] = jnp.broadcast_to(keep_ref[j:j + 1, :], (128, 128)).T

    def out(k, t):
        return pltpu.make_async_copy(zb[k], z_hbm.at[t * nv + k], out_sem.at[k])

    def body(t, carry):
        load_x(t).wait()
        x_blk = x_ref[t]
        for v in range(nv):
            @pl.when(t == 0)
            def _():
                load_e(v).wait()

            @pl.when(t > 0)
            def _():
                out(v, 0).wait()

            at = slice(v * TV, (v + 1) * TV)
            z = lax.dot_general(e_ref[at, :], x_blk, (((1,), (1,)), ((), ())), preferred_element_type=jnp.float32)
            zb[v][...] = z * LOG2E + jnp.concatenate([bias_ref[at, :]] * (TT // 128), axis=1)
            prev = (v - 1) % nv
            t_prev = t if v else jnp.maximum(t - 1, 0)
            base = prev * TV if v else jnp.where(t > 0, prev * TV, -(1 << 30))
            tile_stats(zb[prev], base, t_prev * TT, tgt_ref, m_ref, s_ref, p_ref)
            out(v, t).start()
        return carry

    lax.fori_loop(0, nt, body, 0)
    tile_stats(zb[-1], (nv - 1) * TV, (nt - 1) * TT, tgt_ref, m_ref, s_ref, p_ref)
    for k in range(nv):
        out(k, 0).wait()


def forward(embed, keep, x_all, tgt):
    (v, d), nt = embed.shape, x_all.shape[0]
    t, nv = nt * TT, v // TV
    stat = jax.ShapeDtypeStruct((8, t), jnp.float32)
    return pl.pallas_call(
        forward_kernel,
        out_shape=(jax.ShapeDtypeStruct((nv * nt, TV, TT), jnp.float32), stat, stat, stat),
        in_specs=[ANY, VM, ANY, VM],
        out_specs=(ANY, VM, VM, VM),
        scratch_shapes=[
            pltpu.VMEM((v, d), jnp.bfloat16),
            pltpu.VMEM((nt, TT, d), jnp.bfloat16),
            pltpu.VMEM((v, 128), jnp.float32),
        ]
        + [pltpu.VMEM((TV, TT), jnp.float32)] * nv
        + [pltpu.SemaphoreType.DMA((nv,)), pltpu.SemaphoreType.DMA((nv,)), pltpu.SemaphoreType.DMA((nt,))],
        compiler_params=pltpu.CompilerParams(vmem_limit_bytes=VMEM_LIMIT),
        cost_estimate=pl.CostEstimate(flops=2 * v * t * d, bytes_accessed=4 * v * t, transcendentals=v * t),
        name="logits",
    )(embed, keep, x_all, tgt)


def tile_grad(z_ref, dz_ref, base, col, lse_ref, w_ref, tgt_ref):
    rows, tokens = z_ref.shape
    for c in range(0, tokens, 128):
        at = cols(col + c, 128)
        lse = jnp.broadcast_to(lse_ref[:, at], (8, 128))
        w = jnp.broadcast_to(w_ref[:, at], (8, 128))
        rel = jnp.broadcast_to(tgt_ref[:, at], (8, 128)) - lax.broadcasted_iota(jnp.int32, (8, 128), 0) - base
        for r in range(0, rows, 16):
            pair = []
            for q in (r, r + 8):
                p = jnp.exp2(z_ref[q:q + 8, c:c + 128] - lse)
                pair.append(p - jnp.where(rel == q, w, 0.0))
            dz_ref[r:r + 16, c:c + 128] = jnp.concatenate(pair, axis=0).astype(jnp.bfloat16)


def dx_kernel(et_ref, lse_ref, w_ref, tgt_ref, z_hbm, dx_hbm, *rest):
    nv, nt = et_ref.shape[1] // TV, lse_ref.shape[1] // TT
    n = nv * nt
    zb, db = rest[:nv], rest[nv:nv + 2]
    acc, z_sem, x_sem = rest[nv + 2:]

    def z_in(k, g):
        return pltpu.make_async_copy(z_hbm.at[g], zb[k], z_sem.at[k])

    def x_out(par, t):
        return pltpu.make_async_copy(acc.at[par], dx_hbm.at[t], x_sem.at[par])

    def grad(v, t, d_ref):
        tile_grad(zb[v], d_ref, v * TV, t * TT, lse_ref, w_ref, tgt_ref)

    for k in range(nv):
        z_in(k, k).start()
    for k in range(2):
        x_out(k, k).start()
    z_in(0, 0).wait()
    grad(0, 0, db[0])
    z_in(0, nv).start()

    def block(t, par):
        x_out(par, 0).wait()
        for v in range(nv):
            cur, nxt = db[(par * nv + v) % 2], db[(par * nv + v + 1) % 2]
            vn = (v + 1) % nv
            tn = t if v + 1 < nv else jnp.minimum(t + 1, nt - 1)
            z_in(vn, 0).wait()
            d = jnp.dot(et_ref[:, v * TV:(v + 1) * TV], cur[...], preferred_element_type=jnp.float32)
            acc[par] = d if v == 0 else acc[par] + d
            grad(vn, tn, nxt)
            z_in(vn, jnp.minimum((tn + 1) * nv + vn, n - nv + vn)).start()
        x_out(par, t).start()

    def body(i, carry):
        block(2 * i, 0)
        block(2 * i + 1, 1)
        return carry

    lax.fori_loop(0, nt // 2, body, 0)
    for k in range(nv):
        z_in(k, 0).wait()
    for k in range(2):
        x_out(k, 0).wait()


def token_grad(embed_t, lse, w, tgt, z):
    (d, v), t = embed_t.shape, lse.shape[1]
    nv = v // TV
    return pl.pallas_call(
        dx_kernel,
        out_shape=jax.ShapeDtypeStruct((t // TT, d, TT), jnp.float32),
        in_specs=[VM] * 4 + [ANY],
        out_specs=ANY,
        scratch_shapes=[pltpu.VMEM((TV, TT), jnp.float32)] * nv
        + [pltpu.VMEM((TV, TT), jnp.bfloat16)] * 2
        + [pltpu.VMEM((2, d, TT), jnp.float32), pltpu.SemaphoreType.DMA((nv,)), pltpu.SemaphoreType.DMA((2,))],
        compiler_params=pltpu.CompilerParams(vmem_limit_bytes=VMEM_LIMIT),
        cost_estimate=pl.CostEstimate(flops=2 * v * t * d, bytes_accessed=4 * v * t, transcendentals=v * t),
        name="token_grad",
    )(embed_t, lse, w, tgt, z)


def de_kernel(z_hbm, x_ref, lse_ref, w_ref, tgt_ref, o_hbm, acc, *rest):
    nt = x_ref.shape[0]
    nv = z_hbm.shape[0] // nt
    zb, (z_sem, o_sem) = rest[:4], rest[4:]

    def z_in(k, g):
        v, t = lax.div(g, nt // 4), lax.rem(g, nt // 4) * 4 + k
        return pltpu.make_async_copy(z_hbm.at[t * nv + v], zb[k], z_sem.at[k])

    def o_out(v):
        return pltpu.make_async_copy(acc.at[lax.rem(v, 2)], o_hbm.at[pl.ds(pl.multiple_of(v * TV, TV), TV)], o_sem.at[lax.rem(v, 2)])

    for k in range(4):
        z_in(k, 0).start()
    last = nv * (nt // 4) - 1

    def body(g, carry):
        v, q = lax.div(g, nt // 4), lax.rem(g, nt // 4)
        slot = lax.rem(v, 2)

        @pl.when((q == 0) & (v >= 2))
        def _():
            o_out(v).wait()

        for k in range(4):
            z_in(k, 0).wait()
            t = q * 4 + k
            at = cols(t * TT)
            lse = lse_ref[:, at]
            w = jnp.broadcast_to(w_ref[:, at], (8, TT))
            rel = jnp.broadcast_to(tgt_ref[:, at], (8, TT)) - lax.broadcasted_iota(jnp.int32, (8, TT), 0) - v * TV
            x_blk = x_ref[t, :TT]
            for c in range(0, TV, 256):
                p = jnp.exp2(zb[k][c:c + 256] - lse)
                dz = jnp.concatenate([p[r:r + 8] - jnp.where(rel == c + r, w, 0.0) for r in range(0, 256, 8)], axis=0)
                d = jnp.dot(dz.astype(jnp.bfloat16), x_blk, preferred_element_type=jnp.float32)
                old = acc[slot, c:c + 256]
                acc[slot, c:c + 256] = d + (jnp.where(q == 0, 0.0, old) if k == 0 else old)
            z_in(k, jnp.minimum(g + 1, last)).start()

        @pl.when(q == nt // 4 - 1)
        def _():
            o_out(v).start()

        return carry

    lax.fori_loop(0, last + 1, body, 0)
    for k in range(4):
        z_in(k, 0).wait()
    for v in range(max(nv - 2, 0), nv):
        o_out(v).wait()


def embed_grad(z, x_all, lse, w, tgt, v):
    nt, _, d = x_all.shape
    t = nt * TT
    return pl.pallas_call(
        de_kernel,
        out_shape=jax.ShapeDtypeStruct((v, d), jnp.float32),
        in_specs=[ANY] + [VM] * 4,
        out_specs=ANY,
        scratch_shapes=[pltpu.VMEM((2, TV, d), jnp.float32)]
        + [pltpu.VMEM((TV, TT), jnp.float32)] * 4
        + [pltpu.SemaphoreType.DMA((4,)), pltpu.SemaphoreType.DMA((2,))],
        compiler_params=pltpu.CompilerParams(vmem_limit_bytes=VMEM_LIMIT),
        cost_estimate=pl.CostEstimate(flops=2 * v * t * d, bytes_accessed=4 * v * t + 4 * v * d, transcendentals=v * t),
        name="embed_grad",
    )(z, x_all, lse, w, tgt)


def exchange(slots, me, n, send_sem, recv_sem):
    barrier = pltpu.get_barrier_semaphore()
    peers = [lax.rem(me + k, n) for k in range(1, n)]
    for peer in peers:
        pl.semaphore_signal(barrier, inc=1, device_id={"tp": peer}, device_id_type=pl.DeviceIdType.MESH)
    pl.semaphore_wait(barrier, n - 1)
    copies = [
        pltpu.make_async_remote_copy(
            src_ref=slots.at[me],
            dst_ref=slots.at[me],
            send_sem=send_sem.at[k],
            recv_sem=recv_sem.at[k],
            device_id={"tp": peer},
            device_id_type=pl.DeviceIdType.MESH,
        )
        for k, peer in enumerate(peers)
    ]
    for copy in copies:
        copy.start()
    for copy in copies:
        copy.wait()


def combine_kernel(n, m_ref, s_ref, p_ref, lse_ref, picked_ref, slots, send_sem, recv_sem):
    me = lax.axis_index("tp")
    m = m_ref[...]
    top = jnp.max(m, axis=0, keepdims=True)
    slots[me, 0:1, :] = top
    slots[me, 1:2, :] = jnp.sum(s_ref[...] * jnp.exp2(m - top), axis=0, keepdims=True)
    slots[me, 2:3, :] = jnp.sum(p_ref[...], axis=0, keepdims=True)
    slots[me, 3:4, :] = jnp.zeros_like(top)
    exchange(slots, me, n, send_sem, recv_sem)
    row_max = slots[0, 0:1, :]
    for i in range(1, n):
        row_max = jnp.maximum(row_max, slots[i, 0:1, :])
    total = jnp.zeros_like(row_max)
    picked = jnp.zeros_like(row_max)
    for i in range(n):
        total = total + slots[i, 1:2, :] * jnp.exp2(slots[i, 0:1, :] - row_max)
        picked = picked + slots[i, 2:3, :]
    lse_ref[...] = row_max + jnp.log2(total)
    picked_ref[...] = picked


def combine(m8, s8, p8, n):
    t = m8.shape[1]
    row = jax.ShapeDtypeStruct((1, t), jnp.float32)
    return pl.pallas_call(
        functools.partial(combine_kernel, n),
        out_shape=(row, row),
        in_specs=[VM] * 3,
        out_specs=(VM, VM),
        scratch_shapes=[pltpu.VMEM((n, 4, t), jnp.float32), pltpu.SemaphoreType.DMA((n - 1,)), pltpu.SemaphoreType.DMA((n - 1,))],
        compiler_params=pltpu.CompilerParams(collective_id=0, has_side_effects=True),
        name="combine",
    )(m8, s8, p8)


def norm_grad_kernel(n, h_ref, gamma_ref, dxt_ref, dh_ref, g_ref, slots, send_sem, recv_sem):
    me = lax.axis_index("tp")
    h = h_ref[...].astype(jnp.float32)
    mean = jnp.mean(h, axis=1, keepdims=True)
    cen = h - mean
    rstd = lax.rsqrt(jnp.mean(cen * cen, axis=1, keepdims=True) + LN_EPS)
    xhat = cen * rstd
    dy = dxt_ref[...].T
    d = dy.shape[1]
    slots[me, 0:1, :] = jnp.sum(dy * xhat, axis=0, keepdims=True)
    slots[me, 1:2, :] = jnp.sum(dy, axis=0, keepdims=True)
    slots[me, 2:8, :] = jnp.zeros((6, d), jnp.float32)
    dn = dy * gamma_ref[...]
    dh = rstd * (dn - jnp.mean(dn, axis=1, keepdims=True) - xhat * jnp.mean(dn * xhat, axis=1, keepdims=True))
    dh_ref[...] = dh.astype(jnp.bfloat16)
    exchange(slots, me, n, send_sem, recv_sem)
    total = slots[0]
    for i in range(1, n):
        total = total + slots[i]
    g_ref[...] = total


def norm_grad(hidden, gamma, dx_t, n):
    t, d = hidden.shape
    return pl.pallas_call(
        functools.partial(norm_grad_kernel, n),
        out_shape=(jax.ShapeDtypeStruct((t, d), jnp.bfloat16), jax.ShapeDtypeStruct((8, d), jnp.float32)),
        in_specs=[VM] * 3,
        out_specs=(VM, VM),
        scratch_shapes=[pltpu.VMEM((n, 8, d), jnp.float32), pltpu.SemaphoreType.DMA((n - 1,)), pltpu.SemaphoreType.DMA((n - 1,))],
        compiler_params=pltpu.CompilerParams(collective_id=1, has_side_effects=True, vmem_limit_bytes=VMEM_LIMIT),
        name="norm_grad",
    )(hidden, gamma[None, :], dx_t)


def solution(mesh):
    tok_spec = P(("dp", "tp"))
    row_spec = P(("dp", "tp"), None)
    group = mesh.shape["tp"]

    def local_step(hidden_blk, ln_gamma, ln_beta, embed_blk, valid_blk, tgt_blk, mask_blk):
        tok_local = hidden_blk.shape[0]
        shard_vocab = embed_blk.shape[0]
        shard_idx = lax.axis_index("tp")
        normed = layer_norm(hidden_blk.astype(jnp.float32), ln_gamma, ln_beta)
        label_rows = jnp.stack([tgt_blk // 256, tgt_blk % 256, mask_blk]).astype(jnp.bfloat16)
        label_rows = jnp.pad(label_rows, ((0, 16 - label_rows.shape[0]), (0, hidden_blk.shape[1] - tok_local)))
        packed = jnp.concatenate([normed.astype(jnp.bfloat16), label_rows], axis=0)
        x_all = lax.all_gather(packed, "tp", axis=0)
        labels = x_all[:, tok_local:tok_local + 3, :tok_local].astype(jnp.float32)
        weight = labels[:, 2].reshape(-1)
        tok_count = jnp.sum(weight)
        target_ids = (labels[:, 0] * 256.0 + labels[:, 1]).astype(jnp.int32).reshape(-1)
        tgt = (target_ids - shard_idx * shard_vocab)[None, :]
        keep = jnp.where(valid_blk > 0, 0.0, -jnp.inf).reshape(-1, 128)
        z, m8, s8, p8 = forward(embed_blk, keep, x_all, tgt)
        lse2, picked = combine(m8, s8, p8, group)
        lse2 = lse2[0]
        tok_loss = (lse2 - picked[0]) * LN2 * weight
        mean_loss = (jnp.sum(tok_loss) / tok_count).reshape(1)
        shift = jnp.where(weight > 0, lse2 + jnp.log2(tok_count), jnp.inf)[None, :]
        scale = (weight / tok_count)[None, :]
        dx_part = token_grad(embed_blk.T, shift, scale, tgt, z)
        dx_local = lax.psum_scatter(dx_part, "tp", scatter_dimension=0, tiled=False)
        d_embed = embed_grad(z, x_all, shift, scale, tgt, shard_vocab)
        d_hidden, ln_grads = norm_grad(hidden_blk, ln_gamma, dx_local, group)
        loss_local = lax.dynamic_slice_in_dim(tok_loss, shard_idx * tok_local, tok_local)
        return loss_local, mean_loss, d_hidden, d_embed, ln_grads[0], ln_grads[1]

    return jax.shard_map(local_step, mesh=mesh, in_specs=(row_spec, P(), P(), P("tp", None), P("tp"), tok_spec, tok_spec), out_specs=(tok_spec, P("dp"), row_spec, row_spec, P("dp"), P("dp")), check_vma=False)
```
